256 devices in a mesh: section: 8 (over x, core), expert: 32 (over z, y).
Axes of the slice: x: 4, y: 4, z: 8, core: 2. Of those that a mesh axis runs over, the one named last changes fastest.
Arguments:
- tokens: bfloat16 [4, 1024, 2048], P(None, 'expert'), may hold values from -6 to 6
- attn_norm: float32 [8, 2048], P('section'), may hold values from 0.5 to 2
- moe_norm: float32 [8, 2048], P('section'), may hold values from 0.5 to 2
- query_weight: bfloat16 [8, 2048, 1024], P('section', 'expert'), may hold values from -4 to 4
- key_weight: bfloat16 [8, 2048, 128], P('section', 'expert'), may hold values from -0.125 to 0.125
- value_weight: bfloat16 [8, 2048, 128], P('section', 'expert'), may hold values from -0.125 to 0.125
- out_weight: bfloat16 [8, 1024, 2048], P('section', 'expert'), may hold values from -0.1875 to 0.1875
- gate_proj: bfloat16 [8, 32, 2048, 704], P('section', 'expert'), may hold values from -0.125 to 0.125
- up_proj: bfloat16 [8, 32, 2048, 704], P('section', 'expert'), may hold values from -0.125 to 0.125
- down_proj: bfloat16 [8, 32, 704, 2048], P('section', 'expert'), may hold values from -0.21875 to 0.21875
- routes: int32 [8, 4, 1024, 6], P('section', None, 'expert'), may hold values from 0 to 31, all different within a row; in each aligned block of 32 rows (0 to 31, 32 to 63, ..., all dimensions but the last counted through in order) at most 8 rows name the same one
- weights_code: int32 [8, 4, 1024, 6], P('section', None, 'expert'), may hold values from 8 to 64
Outputs:
- hidden_states: bfloat16 [8, 4, 1024, 2048], P('section', None, 'expert')
The draws below stay inside these ranges and needn't reach their ends.
Inputs may be any that keep to these rules, and one draw needn't show every extreme that they name: `routes`: each row names 6 different experts. In each aligned block of 32 rows (one sequence's tokens of one micro-batch of one layer) no expert is named by more than 8 rows, a bound that some block reaches.
All inputs are finite; a program needn't handle non-finite values.
Results may differ from the reference program's by a relative error of at most 0.03.
Values may be sent and summed in bfloat16 or wider, within the bound.
No kernel may reach another device: no remote copies, remote signals or barrier semaphores. Data moves between devices by JAX's collectives and lax.ppermute only.
A program may use at most 128 MiB of HBM per device.

```python
import math
import jax
import jax.numpy as jnp
import numpy as np
from jax import lax

D = 2048
FF = 704
HEADS = 8
HEAD_WIDTH = 128
TOP = 6
MICRO = 4
TOK_DEV = 32
LAYERS = 8
EXPERTS = 32
SEQ = 128
TOKENS = 1024
CAP = 8
N_EXPERT = 32


def attention_draw(key):
    base_key = jax.random.fold_in(key, 31)
    first_key, second_key = jax.random.split(base_key, 2)
    key_part = jax.random.normal(first_key, (LAYERS, D, HEAD_WIDTH), jnp.float32) / jnp.sqrt(jnp.float32(D))
    key_part = jnp.clip(key_part, -0.125, 0.125)
    noise_part = jax.random.normal(second_key, (LAYERS, D, HEADS * HEAD_WIDTH), jnp.float32) / jnp.sqrt(jnp.float32(D))
    query_part = noise_part
    return (jnp.clip(query_part, -4.0, 4.0), key_part)


def draw_query_weight(key, part):
    return attention_draw(key)[0].astype(jnp.bfloat16)


def draw_key_weight(key, part):
    return attention_draw(key)[1].astype(jnp.bfloat16)


def with_ends(result, own_key, least, high):
    place = [jax.random.randint(jax.random.fold_in(own_key, axis), (), 0, length) for axis, length in enumerate(result.shape)]
    longest = result.shape.index(max(result.shape))
    neighbour = place[:longest] + [(place[longest] + 1) % result.shape[longest]] + place[longest + 1:]
    return result.at[tuple(place)].set(least).at[tuple(neighbour)].set(high)


def shard_levels(stream_key, dims, cuts, smallest, top_value):
    level, own = 1.0, jax.random.fold_in(stream_key, 6)
    for dim, parts in cuts:
        draws = jnp.exp(jax.random.uniform(jax.random.fold_in(own, dim), (parts,), jnp.float32, smallest / len(cuts), top_value / len(cuts)))
        level = level * jnp.repeat(draws, dims[dim] // parts).reshape([-1 if axis == dim else 1 for axis in range(len(dims))])
    return level


def deal_out(stream_key, own, number, rows, amount, top, limit, slope):
    ranking = jax.random.permutation(stream_key, amount)
    crowded, usual = shares(amount, rows * top, limit, slope, True), shares(amount, rows * top, limit, slope, False)
    places = jnp.arange(amount)

    def named(lengths, rotation):
        used = int((lengths > 0).sum())
        fixed = max(1, used // 4)
        passed = fixed + (places - fixed + rotation * (used - fixed)) % max(1, amount - fixed)
        return jnp.zeros((amount,), jnp.int32).at[ranking[jnp.where(places < fixed, places, passed)]].set(jnp.asarray(lengths, jnp.int32))

    lengths = jnp.where(number % 4 == 0, named(crowded, number // 4), named(usual, number - number // 4 - 1))
    mixed = jax.random.permutation(jax.random.fold_in(own, 3), amount)
    giver, receiver = mixed[0:amount // 2 * 2:2], mixed[1:amount // 2 * 2:2]
    slack = jnp.minimum(lengths[giver] - 1, limit - lengths[receiver]) // 2
    slack = jnp.where((giver == ranking[0]) | (receiver == ranking[0]) | (lengths[receiver] == 0), 0, jnp.maximum(slack, 0))
    passed = jax.random.randint(jax.random.fold_in(own, 4), (amount // 2,), 0, 1 << 20) % (slack + 1)
    lengths = lengths.at[giver].add(-passed).at[receiver].add(passed)
    members = jnp.searchsorted(jnp.cumsum(lengths), jnp.arange(rows * top), side="right").astype(jnp.int32)
    grid = members.reshape(top, rows).T
    grid = grid[jax.random.permutation(jax.random.fold_in(own, 1), rows)]
    rotation = jax.random.randint(jax.random.fold_in(own, 2), (rows, 1), 0, top)
    return jnp.take_along_axis(grid, (jnp.arange(top)[None, :] + rotation) % top, axis=1)


def shares(number_of, total, reach, lean, full):
    loads = [(1 << 20) // math.isqrt(standing ** lean) + 1 for standing in range(1, number_of + 1)]
    largest = reach if full else min(reach, max(-(-total // number_of), total * loads[0] // sum(loads)))
    least = 1 if total - largest >= number_of - 1 else 0
    given, spare = [largest] + [least] * (number_of - 1), total - largest - least * (number_of - 1)
    while spare > 0:
        candidates = [i for i in range(1, number_of) if given[i] < largest] or [i for i in range(1, number_of) if given[i] < reach]
        mass, left = sum([loads[i] for i in candidates]), spare
        for i in candidates:
            extra = min(reach - given[i], max(1, left * loads[i] // mass), spare)
            given[i] = given[i] + extra
            spare = spare - extra
    return np.array(given)


def noise(rng, dims, width, limit, pieces=(), held_as=jnp.bfloat16):
    factor_of = shard_levels(rng, dims, pieces, -0.22, 0.18) if pieces else 1.0
    values = jax.random.normal(rng, dims, jnp.float32) * width * factor_of
    return jnp.minimum(jnp.maximum(values, -limit), limit).astype(held_as)


def setup_inputs(seed: int = 0) -> dict:
    seeds = jax.random.split(jax.random.key(seed), 13)
    tokens = noise(seeds[0], (MICRO, TOKENS, D), 1.0, 6.0, ((1, 32),))
    attn_norm = jnp.clip(jnp.exp(math.log(2.0) - 1.3862944 * jax.random.uniform(seeds[1], (LAYERS, D), jnp.float32) ** shard_levels(seeds[1], (LAYERS, D), ((0, 8),), -0.2, 0.2)), 0.5, 2.0)
    moe_norm = jnp.clip(jnp.exp(math.log(2.0) - 1.3862944 * jax.random.uniform(seeds[2], (LAYERS, D), jnp.float32) ** shard_levels(seeds[2], (LAYERS, D), ((0, 8),), -0.2, 0.2)), 0.5, 2.0)
    query_weight = draw_query_weight(jax.random.fold_in(seeds[12], 71), 0)
    key_weight = draw_key_weight(jax.random.fold_in(seeds[12], 71), 0)
    value_weight = noise(seeds[5], (LAYERS, D, HEAD_WIDTH), D ** -0.5, 0.125, ((0, 8), (1, 32)))
    out_weight = noise(seeds[6], (LAYERS, HEADS * HEAD_WIDTH, D), (HEADS * HEAD_WIDTH) ** -0.5, 0.1875, ((0, 8), (1, 32)))
    gate_proj = noise(seeds[7], (LAYERS, EXPERTS, D, FF), D ** -0.5, 0.125, ((0, 8), (1, 32)))
    up_proj = noise(seeds[8], (LAYERS, EXPERTS, D, FF), D ** -0.5, 0.125, ((0, 8), (1, 32)))
    down_proj = noise(seeds[9], (LAYERS, EXPERTS, FF, D), FF ** -0.5, 0.21875, ((0, 8), (1, 32)))
    routes_keys = jax.random.split(jax.random.fold_in(seeds[10], 1), LAYERS * MICRO * TOKENS // TOK_DEV)
    routes_turns = jax.random.permutation(jax.random.fold_in(seeds[10], 3), LAYERS * MICRO * TOKENS // TOK_DEV)
    routes = jax.vmap(lambda own, number: deal_out(jax.random.fold_in(seeds[10], 2), own, number, TOK_DEV, EXPERTS, TOP, CAP, 1))(routes_keys, routes_turns).reshape((LAYERS, MICRO, TOKENS, TOP))
    weights_code = with_ends(jax.random.randint(seeds[11], (LAYERS, MICRO, TOKENS, TOP), 8, 65), jax.random.fold_in(seeds[11], 1), 8, 64).astype(jnp.int32)
    return {"tokens": tokens, "attn_norm": attn_norm, "moe_norm": moe_norm, "query_weight": query_weight, "key_weight": key_weight, "value_weight": value_weight, "out_weight": out_weight, "gate_proj": gate_proj, "up_proj": up_proj, "down_proj": down_proj, "routes": routes, "weights_code": weights_code}


epsilon = 1e-06

def rms_scale(features, gain_vector):
    return features * lax.rsqrt(lax.optimization_barrier(jnp.mean(features * features, axis=-1, keepdims=True)) + epsilon) * gain_vector

def expert_rows(slot_rows, gate_matrix, up_matrix, down_matrix):
    gated = jnp.dot(slot_rows, gate_matrix, preferred_element_type=jnp.float32)
    lifted = jnp.dot(slot_rows, up_matrix, preferred_element_type=jnp.float32)
    hidden = (jax.nn.silu(gated) * lifted).astype(jnp.bfloat16)
    return jnp.dot(hidden, down_matrix, preferred_element_type=jnp.float32).astype(jnp.bfloat16)

def apply_expert(expert_item):
    return expert_rows(expert_item[0], expert_item[1], expert_item[2], expert_item[3])

def mixture(normed, picks, codes, gate_all, up_all, down_all):
    assigned = picks.reshape(-1).astype(jnp.int32)
    assigned_count = assigned.shape[0]
    ordering = jnp.argsort(assigned, stable=True).astype(jnp.int32)
    sorted_ids = assigned[ordering]
    counts = lax.optimization_barrier(jnp.sum((assigned[:, None] == jnp.arange(EXPERTS, dtype=jnp.int32)[None, :]).astype(jnp.int32), axis=0))
    starts = jnp.cumsum(counts).astype(jnp.int32) - counts
    bound_rows = CAP * N_EXPERT
    slot_ranks = jnp.arange(assigned_count, dtype=jnp.int32) - starts[sorted_ids]
    places = sorted_ids * bound_rows + slot_ranks
    source_rows = normed[ordering // TOP]
    buffer = jnp.zeros((EXPERTS * bound_rows, D), normed.dtype).at[places].set(source_rows)
    buffer = buffer.reshape(EXPERTS, bound_rows, D)
    outputs = lax.map(apply_expert, (buffer, gate_all, up_all, down_all))
    results = outputs.reshape(EXPERTS * bound_rows, D)[places]
    unsorted = jnp.zeros_like(results).at[ordering].set(results)
    pick_weights = codes.astype(jnp.float32) / 64.0
    return lax.optimization_barrier(jnp.sum(unsorted.astype(jnp.float32).reshape(-1, TOP, D) * pick_weights[:, :, None], axis=1))

def attention(sequences, gain_vector, query_matrix, key_matrix, value_matrix, out_matrix):
    normed = rms_scale(sequences.astype(jnp.float32), gain_vector).astype(jnp.bfloat16)
    flat_rows = normed.reshape(-1, D)
    query_rows = jnp.dot(flat_rows, query_matrix, preferred_element_type=jnp.float32).astype(jnp.bfloat16)
    query_rows = query_rows.reshape(N_EXPERT, SEQ, HEADS, HEAD_WIDTH)
    key_vectors = jnp.dot(flat_rows, key_matrix, preferred_element_type=jnp.float32).astype(jnp.bfloat16)
    key_vectors = key_vectors.reshape(N_EXPERT, SEQ, HEAD_WIDTH)
    value_vectors = jnp.dot(flat_rows, value_matrix, preferred_element_type=jnp.float32).astype(jnp.bfloat16)
    value_vectors = value_vectors.reshape(N_EXPERT, SEQ, HEAD_WIDTH)
    attention_scores = jnp.einsum('coal,cjl->caoj', query_rows.astype(jnp.float32), key_vectors.astype(jnp.float32)) * HEAD_WIDTH ** (-0.5)
    positions = jnp.arange(SEQ, dtype=jnp.int32)
    causal = positions[None, :] <= positions[:, None]
    attention_scores = jnp.where(causal[None, None], attention_scores, -1e+30)
    highest = lax.optimization_barrier(jnp.max(attention_scores, axis=-1, keepdims=True))
    exponent = jnp.exp(attention_scores - highest)
    attention_probabilities = (exponent / lax.optimization_barrier(jnp.sum(exponent, axis=-1, keepdims=True))).astype(jnp.bfloat16)
    attended_values = jnp.einsum('xmpo,xot->xpmt', attention_probabilities.astype(jnp.float32), value_vectors.astype(jnp.float32))
    attended_values = attended_values.astype(jnp.bfloat16).reshape(-1, HEADS * HEAD_WIDTH)
    return jnp.dot(attended_values, out_matrix, preferred_element_type=jnp.float32).reshape(N_EXPERT, SEQ, D)

def reference(tokens, attn_norm, moe_norm, query_weight, key_weight, value_weight, out_weight, gate_proj, up_proj, down_proj, routes, weights_code):
    current = tokens
    layer_outputs = []
    for layer_index in range(LAYERS):
        sequences = current.reshape(MICRO, N_EXPERT, TOK_DEV, D).transpose(1, 0, 2, 3).reshape(N_EXPERT, SEQ, D)
        attended = attention(sequences, attn_norm[layer_index], query_weight[layer_index], key_weight[layer_index], value_weight[layer_index], out_weight[layer_index])
        attended = attended.reshape(N_EXPERT, MICRO, TOK_DEV, D).transpose(1, 0, 2, 3).reshape(MICRO * TOKENS, D)
        flat_input = current.reshape(-1, D).astype(jnp.float32)
        normed = rms_scale(flat_input, moe_norm[layer_index]).astype(jnp.bfloat16)
        gate_all = gate_proj[layer_index]
        up_all = up_proj[layer_index]
        down_all = down_proj[layer_index]

        def micro_mixture(micro_item):
            return mixture(micro_item[0], micro_item[1], micro_item[2], gate_all, up_all, down_all)
        mixed = lax.map(micro_mixture, (normed.reshape(MICRO, TOKENS, D), routes[layer_index], weights_code[layer_index]))
        mixed = mixed.reshape(MICRO * TOKENS, D)
        current = (flat_input + attended + mixed).astype(jnp.bfloat16).reshape(MICRO, TOKENS, D)
        layer_outputs.append(current)
    return jnp.stack(layer_outputs)
```

```python
import jax
import jax.numpy as jnp
from jax import lax
from jax.experimental import pallas as pl
from jax.experimental.pallas import tpu as pltpu
from jax.sharding import PartitionSpec as P

epsilon = 1e-06

POSITION = (0, 6, 2, 4, 7, 3, 1, 5)
LAYER_AT = tuple(POSITION.index(place) for place in range(8))
MOVES = [(layer, place) for layer, place in enumerate(POSITION) if layer != place]
HOME = [(place, layer) for layer, place in MOVES]
RELAY = [(POSITION[layer], POSITION[layer + 1]) for layer in range(7)]

CHUNKS = 4


def rms_normed(wide, gain_vector):
    scale = lax.rsqrt(jnp.mean(wide * wide, axis=-1, keepdims=True) + epsilon)
    return (wide * scale * gain_vector).astype(jnp.bfloat16)


def expert_kernel(
    moved_ref,
    rows_ref,
    gate_own,
    up_own,
    down_own,
    gate_new,
    up_new,
    down_new,
    out_ref,
    gate_buf,
    up_buf,
    down_buf,
    gate_acc,
    up_acc,
    gate_sem,
    up_sem,
    down_sem,
):
    depth = gate_buf.shape[1]
    width = down_buf.shape[2]

    def copies(gate_hbm, up_hbm, down_hbm):
        firsts, lasts = [], []
        for step in range(CHUNKS):
            part = pl.ds(step * depth, depth)
            firsts.append(
                (
                    pltpu.make_async_copy(
                        gate_hbm.at[part, :], gate_buf.at[step], gate_sem.at[step]
                    ),
                    pltpu.make_async_copy(up_hbm.at[part, :], up_buf.at[step], up_sem.at[step]),
                )
            )
        for step in range(CHUNKS):
            part = pl.ds(step * width, width)
            lasts.append(
                pltpu.make_async_copy(down_hbm.at[:, part], down_buf.at[step], down_sem.at[step])
            )
        return firsts, lasts

    def start(firsts, lasts):
        for first, second in firsts:
            first.start()
            second.start()
        for copy in lasts:
            copy.start()

    moved = moved_ref[0]

    @pl.when(moved == 0)
    def _():
        start(*copies(gate_own, up_own, down_own))

    @pl.when(moved != 0)
    def _():
        start(*copies(gate_new, up_new, down_new))

    firsts, lasts = copies(gate_own, up_own, down_own)
    for step in range(CHUNKS):
        first, second = firsts[step]
        rows = rows_ref[:, step * depth : (step + 1) * depth]
        first.wait()
        gated = jnp.dot(rows, gate_buf[step], preferred_element_type=jnp.float32)
        second.wait()
        lifted = jnp.dot(rows, up_buf[step], preferred_element_type=jnp.float32)
        if step == 0:
            gate_acc[...] = gated
            up_acc[...] = lifted
        else:
            gate_acc[...] += gated
            up_acc[...] += lifted
    gated = gate_acc[...]
    hidden = (gated * jax.nn.sigmoid(gated) * up_acc[...]).astype(jnp.bfloat16)
    for step in range(CHUNKS):
        lasts[step].wait()
        out_ref[:, step * width : (step + 1) * width] = jnp.dot(
            hidden, down_buf[step], preferred_element_type=jnp.float32
        ).astype(jnp.bfloat16)


def expert_rows(moved, rows, own, new):
    count, model_width = rows.shape
    hidden_width = own[0].shape[1]
    depth = model_width // CHUNKS
    vmem = pl.BlockSpec(memory_space=pltpu.VMEM)
    anywhere = pl.BlockSpec(memory_space=pl.ANY)
    return pl.pallas_call(
        expert_kernel,
        out_shape=jax.ShapeDtypeStruct((count, model_width), jnp.bfloat16),
        in_specs=[pl.BlockSpec(memory_space=pltpu.SMEM), vmem] + [anywhere] * 6,
        out_specs=vmem,
        scratch_shapes=[
            pltpu.VMEM((CHUNKS, depth, hidden_width), jnp.bfloat16),
            pltpu.VMEM((CHUNKS, depth, hidden_width), jnp.bfloat16),
            pltpu.VMEM((CHUNKS, hidden_width, depth), jnp.bfloat16),
            pltpu.VMEM((count, hidden_width), jnp.float32),
            pltpu.VMEM((count, hidden_width), jnp.float32),
            pltpu.SemaphoreType.DMA((CHUNKS,)),
            pltpu.SemaphoreType.DMA((CHUNKS,)),
            pltpu.SemaphoreType.DMA((CHUNKS,)),
        ],
        compiler_params=pltpu.CompilerParams(vmem_limit_bytes=40 * 2**20),
        cost_estimate=pl.CostEstimate(
            flops=6 * count * model_width * hidden_width,
            bytes_accessed=6 * model_width * hidden_width + 4 * count * model_width,
            transcendentals=count * hidden_width,
        ),
        name="experts",
    )(moved, rows, *own, *new)


def route_tables(picks, codes, expert_count, capacity):
    micro_count, tok_rows, pick_count = picks.shape
    flat_ids = picks.reshape(micro_count, tok_rows * pick_count)
    experts = jnp.arange(expert_count, dtype=jnp.int32)
    matches = (flat_ids[:, :, None] == experts[None, None, :]).astype(jnp.float32)
    order = jnp.arange(tok_rows * pick_count, dtype=jnp.int32)
    earlier = (order[:, None] > order[None, :]).astype(jnp.float32)
    before = jnp.einsum("ij,mje->mie", earlier, matches)
    slot_ranks = jnp.sum(before * matches, axis=2).astype(jnp.int32)
    columns = (flat_ids * capacity + slot_ranks).reshape(micro_count, tok_rows, pick_count)
    slots = jnp.arange(expert_count * capacity, dtype=jnp.int32)
    pick_weights = codes.astype(jnp.float32) / 64.0
    scatter_table = jnp.zeros((micro_count, tok_rows, expert_count * capacity), jnp.float32)
    combine_table = scatter_table
    for pick in range(pick_count):
        onehot = (columns[:, :, pick, None] == slots[None, None, :]).astype(jnp.float32)
        scatter_table = scatter_table + onehot
        combine_table = combine_table + onehot * pick_weights[:, :, pick, None]
    return (scatter_table.astype(jnp.bfloat16), combine_table.astype(jnp.bfloat16))


def shards(
    tokens,
    attn_norm,
    moe_norm,
    query_weight,
    key_weight,
    value_weight,
    out_weight,
    gate_proj,
    up_proj,
    down_proj,
    routes,
    weights_code,
):
    section_count = lax.axis_size("section")
    place = lax.axis_index("section")
    expert_devices = lax.axis_size("expert")
    micro_count, tok_rows, model_width = tokens.shape
    pick_count = routes.shape[3]
    expert_count = expert_devices * gate_proj.shape[1]
    capacity = min(tok_rows, tok_rows * pick_count * 4 // (3 * expert_count))
    layer = jnp.asarray(LAYER_AT, jnp.int32)[place]
    here = layer == place
    moved = (layer != place).astype(jnp.int32).reshape(1)

    def relocated(value):
        return jnp.where(here, value, lax.ppermute(value, "section", MOVES))

    head_size = key_weight.shape[-1]
    head_count = query_weight.shape[-1] // head_size
    half = model_width // 2
    out_shard = out_weight[0]
    packed = jnp.concatenate(
        [
            query_weight[0],
            key_weight[0],
            value_weight[0],
            jnp.concatenate([out_shard[:, :half], out_shard[:, half:]], axis=0),
        ],
        axis=1,
    )
    full = lax.all_gather(relocated(packed), "expert", axis=0, tiled=True)
    tables = relocated(jnp.concatenate([routes[0], weights_code[0]], axis=-1))
    gains = relocated(jnp.concatenate([attn_norm, moe_norm], axis=0))
    attn_gain, moe_gain = gains[0], gains[1]
    scatter_tables, combine_tables = route_tables(
        tables[:, :, :pick_count], tables[:, :, pick_count:], expert_count, capacity
    )
    own = (gate_proj[0, 0], up_proj[0, 0], down_proj[0, 0])
    new = tuple(lax.ppermute(value, "section", MOVES) for value in own)

    score_width = (head_count + 2) * head_size
    length = micro_count * tok_rows
    score_scale = head_size ** (-0.5)

    def attention_weights(full):
        rows = out_shard.shape[0]
        halves = full[:, score_width:].reshape(expert_devices, 2, rows, half)
        halves = halves.transpose(0, 2, 1, 3).reshape(expert_devices * rows, model_width)
        return (full[:, :score_width], halves)

    def mixture(layer_input, block, own, new, moved):
        wide = layer_input.astype(jnp.float32)
        normed = rms_normed(wide, moe_gain)
        scatter_table = lax.dynamic_index_in_dim(scatter_tables, block, 0, keepdims=False)
        combine_table = lax.dynamic_index_in_dim(combine_tables, block, 0, keepdims=False)
        outgoing = jnp.einsum("te,td->ed", scatter_table, normed, preferred_element_type=jnp.float32)
        outgoing = outgoing.astype(jnp.bfloat16).reshape(expert_count, capacity, model_width)
        arrived = lax.all_to_all(outgoing, "expert", split_axis=0, concat_axis=0, tiled=True)
        produced = expert_rows(moved, arrived.reshape(-1, model_width), own, new)
        produced = produced.reshape(arrived.shape)
        returned = lax.all_to_all(produced, "expert", split_axis=0, concat_axis=0, tiled=True)
        return jnp.dot(
            combine_table, returned.reshape(-1, model_width), preferred_element_type=jnp.float32
        )

    def attend(layer_input, block, old_keys, old_values, inner, outer):
        normed = rms_normed(layer_input.astype(jnp.float32), attn_gain)
        projected = jnp.dot(normed, inner, preferred_element_type=jnp.float32)
        projected = projected.astype(jnp.bfloat16)
        query_rows = projected[:, : head_count * head_size]
        query_rows = query_rows.reshape(tok_rows, head_count, head_size)
        new_keys = projected[:, head_count * head_size : (head_count + 1) * head_size]
        new_values = projected[:, (head_count + 1) * head_size :]
        offset = block * tok_rows
        key_vectors = lax.dynamic_update_slice_in_dim(old_keys, new_keys, offset, 0)
        value_vectors = lax.dynamic_update_slice_in_dim(old_values, new_values, offset, 0)
        scores = jnp.einsum(
            "qhd,kd->hqk", query_rows, key_vectors, preferred_element_type=jnp.float32
        )
        scores = scores * score_scale
        positions = offset + jnp.arange(tok_rows, dtype=jnp.int32)
        causal = jnp.arange(length, dtype=jnp.int32)[None, :] <= positions[:, None]
        scores = jnp.where(causal[None], scores, -1e30)
        highest = jnp.max(scores, axis=-1, keepdims=True)
        exponent = jnp.exp(scores - highest)
        probabilities = exponent / jnp.sum(exponent, axis=-1, keepdims=True)
        context = jnp.einsum(
            "hqk,kd->qhd",
            probabilities.astype(jnp.bfloat16),
            value_vectors,
            preferred_element_type=jnp.float32,
        )
        context = context.astype(jnp.bfloat16).reshape(tok_rows, head_count * head_size)
        attended = jnp.dot(context, outer, preferred_element_type=jnp.float32)
        return (attended, key_vectors, value_vectors)

    keys = jnp.zeros((length, head_size), jnp.bfloat16)
    values = jnp.zeros((length, head_size), jnp.bfloat16)
    leading = layer == 0
    first_block = jnp.int32(0)
    first_rows = tokens[0]
    mixed = lax.cond(
        leading,
        lambda rows: mixture(rows, first_block, own, own, jnp.zeros((1,), jnp.int32)),
        lambda rows: jnp.zeros((tok_rows, model_width), jnp.float32),
        first_rows,
    )
    inner, outer = attention_weights(full)

    def first_attend(arrays):
        rows, mixed, keys, values = arrays
        attended, keys, values = attend(rows, first_block, keys, values, inner, outer)
        output_rows = (rows.astype(jnp.float32) + attended + mixed).astype(jnp.bfloat16)
        return (output_rows, keys, values)

    output_rows, keys, values = lax.cond(
        leading,
        first_attend,
        lambda arrays: (arrays[0], arrays[2], arrays[3]),
        (first_rows, mixed, keys, values),
    )
    tick_count = micro_count + section_count - 1
    stored = jnp.zeros((tick_count, tok_rows, model_width), jnp.bfloat16)
    stored = lax.dynamic_update_index_in_dim(stored, output_rows, 0, 0)
    inbound = lax.ppermute(output_rows, "section", RELAY)

    def advance(tick_index, state_carry):
        inbound, keys, values, stored = state_carry
        block_index = tick_index - layer
        active = (block_index >= 0) & (block_index < micro_count)
        block = jnp.clip(block_index, 0, micro_count - 1)

        def work(arrays):
            inbound, keys, values = arrays
            held = lax.dynamic_index_in_dim(tokens, block, 0, keepdims=False)
            layer_input = jnp.where(layer == 0, held, inbound)
            mixed = mixture(layer_input, block, own, new, moved)
            attended, keys, values = attend(layer_input, block, keys, values, inner, outer)
            output_rows = layer_input.astype(jnp.float32) + attended + mixed
            return (output_rows.astype(jnp.bfloat16), keys, values)

        output_rows, keys, values = lax.cond(
            active, work, lambda arrays: arrays, (inbound, keys, values)
        )
        stored = lax.dynamic_update_index_in_dim(stored, output_rows, tick_index, 0)
        inbound = lax.ppermute(output_rows, "section", RELAY)
        return (inbound, keys, values, stored)

    finals = lax.fori_loop(1, tick_count, advance, (inbound, keys, values, stored))
    results = lax.dynamic_slice_in_dim(finals[3], layer, micro_count, 0)
    returned_home = lax.ppermute(results, "section", HOME)
    return jnp.where(here, results, returned_home)[None]


def solution(mesh):
    placed = (
        P(None, "expert", None),
        P("section", None),
        P("section", None),
        P("section", "expert", None),
        P("section", "expert", None),
        P("section", "expert", None),
        P("section", "expert", None),
        P("section", "expert", None, None),
        P("section", "expert", None, None),
        P("section", "expert", None, None),
        P("section", None, "expert", None),
        P("section", None, "expert", None),
    )
    return jax.shard_map(
        shards,
        mesh=mesh,
        in_specs=placed,
        out_specs=P("section", None, "expert", None),
        check_vma=False,
    )
```

```python
import jax
import jax.numpy as jnp
from jax import lax
from jax.experimental import pallas as pl
from jax.experimental.pallas import tpu as pltpu
from jax.sharding import PartitionSpec as P

epsilon = 1e-06

POSITION = (0, 6, 2, 4, 7, 3, 1, 5)
LAYER_AT = tuple(POSITION.index(place) for place in range(8))
MOVES = [(layer, place) for layer, place in enumerate(POSITION) if layer != place]
HOME = [(place, layer) for layer, place in MOVES]
RELAY = [(POSITION[layer], POSITION[layer + 1]) for layer in range(7)]

def rms_normed(wide, gain_vector):
    scale = lax.rsqrt(jnp.mean(wide * wide, axis=-1, keepdims=True) + epsilon)
    return (wide * scale * gain_vector).astype(jnp.bfloat16)


def expert_kernel(rows_ref, gate_ref, up_ref, down_ref, out_ref):
    rows = rows_ref[...]
    across = (((1,), (1,)), ((), ()))
    gated = lax.dot_general(rows, gate_ref[...], across, preferred_element_type=jnp.float32)
    lifted = lax.dot_general(rows, up_ref[...], across, preferred_element_type=jnp.float32)
    hidden = (gated * jax.nn.sigmoid(gated) * lifted).astype(jnp.bfloat16)
    out_ref[...] = jnp.dot(hidden, down_ref[...], preferred_element_type=jnp.float32).astype(
        jnp.bfloat16
    )


def expert_rows(rows, matrices):
    count, model_width = rows.shape
    hidden_width = matrices[2].shape[0]
    vmem = pl.BlockSpec(memory_space=pltpu.VMEM)
    return pl.pallas_call(
        expert_kernel,
        out_shape=jax.ShapeDtypeStruct((count, model_width), jnp.bfloat16),
        in_specs=[vmem] * 4,
        out_specs=vmem,
        compiler_params=pltpu.CompilerParams(vmem_limit_bytes=24 * 2**20),
        cost_estimate=pl.CostEstimate(
            flops=6 * count * model_width * hidden_width,
            bytes_accessed=6 * model_width * hidden_width + 4 * count * model_width,
            transcendentals=count * hidden_width,
        ),
        name="experts",
    )(rows, *matrices)


def route_tables(picks, codes, expert_count, capacity):
    micro_count, tok_rows, pick_count = picks.shape
    flat_ids = picks.reshape(micro_count, tok_rows * pick_count)
    experts = jnp.arange(expert_count, dtype=jnp.int32)
    matches = (flat_ids[:, :, None] == experts[None, None, :]).astype(jnp.float32)
    order = jnp.arange(tok_rows * pick_count, dtype=jnp.int32)
    earlier = (order[:, None] > order[None, :]).astype(jnp.float32)
    before = jnp.einsum("ij,mje->mie", earlier, matches)
    slot_ranks = jnp.sum(before * matches, axis=2).astype(jnp.int32)
    columns = (flat_ids * capacity + slot_ranks).reshape(micro_count, tok_rows, pick_count)
    slots = jnp.arange(expert_count * capacity, dtype=jnp.int32)
    pick_weights = codes.astype(jnp.float32) / 64.0
    scatter_table = jnp.zeros((micro_count, tok_rows, expert_count * capacity), jnp.float32)
    combine_table = scatter_table
    for pick in range(pick_count):
        onehot = (columns[:, :, pick, None] == slots[None, None, :]).astype(jnp.float32)
        scatter_table = scatter_table + onehot
        combine_table = combine_table + onehot * pick_weights[:, :, pick, None]
    return (scatter_table.astype(jnp.bfloat16), combine_table.astype(jnp.bfloat16))


def shards(
    tokens,
    attn_norm,
    moe_norm,
    query_weight,
    key_weight,
    value_weight,
    out_weight,
    gate_proj,
    up_proj,
    down_proj,
    routes,
    weights_code,
):
    section_count = lax.axis_size("section")
    place = lax.axis_index("section")
    expert_devices = lax.axis_size("expert")
    micro_count, tok_rows, model_width = tokens.shape
    pick_count = routes.shape[3]
    expert_count = expert_devices * gate_proj.shape[1]
    capacity = min(tok_rows, tok_rows * pick_count * 4 // (3 * expert_count))
    layer = jnp.asarray(LAYER_AT, jnp.int32)[place]
    here = layer == place

    def relocated(value):
        return jnp.where(here, value, lax.ppermute(value, "section", MOVES))

    head_size = key_weight.shape[-1]
    head_count = query_weight.shape[-1] // head_size
    half = model_width // 2
    out_shard = out_weight[0]
    packed = jnp.concatenate(
        [
            query_weight[0],
            key_weight[0],
            value_weight[0],
            jnp.concatenate([out_shard[:, :half], out_shard[:, half:]], axis=0),
        ],
        axis=1,
    )
    full = lax.all_gather(relocated(packed), "expert", axis=0, tiled=True)
    tables = relocated(jnp.concatenate([routes[0], weights_code[0]], axis=-1))
    gains = relocated(jnp.concatenate([attn_norm, moe_norm], axis=0))
    attn_gain, moe_gain = gains[0], gains[1]
    scatter_tables, combine_tables = route_tables(
        tables[:, :, :pick_count], tables[:, :, pick_count:], expert_count, capacity
    )
    scatter_tables, combine_tables = lax.optimization_barrier((scatter_tables, combine_tables))
    own = (gate_proj[0, 0].T, up_proj[0, 0].T, down_proj[0, 0])
    here_matrices = tuple(relocated(value) for value in own)

    score_width = (head_count + 2) * head_size
    length = micro_count * tok_rows
    score_scale = head_size ** (-0.5)

    def attention_weights(full):
        rows = out_shard.shape[0]
        halves = full.reshape(expert_devices, 2, rows, score_width + half)
        outer = tuple(
            halves[:, side, :, score_width:].reshape(expert_devices * rows, half)
            for side in range(2)
        )
        return (full[:, :score_width], outer)

    def mixture(layer_input, block, matrices):
        wide = layer_input.astype(jnp.float32)
        normed = rms_normed(wide, moe_gain)
        scatter_table = lax.dynamic_index_in_dim(scatter_tables, block, 0, keepdims=False)
        combine_table = lax.dynamic_index_in_dim(combine_tables, block, 0, keepdims=False)
        outgoing = jnp.einsum("te,td->ed", scatter_table, normed, preferred_element_type=jnp.float32)
        outgoing = outgoing.astype(jnp.bfloat16).reshape(expert_count, capacity, model_width)
        arrived = lax.all_to_all(outgoing, "expert", split_axis=0, concat_axis=0, tiled=True)
        produced = expert_rows(arrived.reshape(-1, model_width), matrices)
        produced = produced.reshape(arrived.shape)
        returned = lax.all_to_all(produced, "expert", split_axis=0, concat_axis=0, tiled=True)
        return jnp.dot(
            combine_table, returned.reshape(-1, model_width), preferred_element_type=jnp.float32
        )

    def attend(layer_input, block, old_keys, old_values, inner, outer):
        normed = rms_normed(layer_input.astype(jnp.float32), attn_gain)
        projected = jnp.dot(normed, inner, preferred_element_type=jnp.float32)
        projected = projected.astype(jnp.bfloat16)
        query_rows = projected[:, : head_count * head_size]
        query_rows = query_rows.reshape(tok_rows, head_count, head_size)
        new_keys = projected[:, head_count * head_size : (head_count + 1) * head_size]
        new_values = projected[:, (head_count + 1) * head_size :]
        offset = block * tok_rows
        key_vectors = lax.dynamic_update_slice_in_dim(old_keys, new_keys, offset, 0)
        value_vectors = lax.dynamic_update_slice_in_dim(old_values, new_values, offset, 0)
        scores = jnp.einsum(
            "qhd,kd->hqk", query_rows, key_vectors, preferred_element_type=jnp.float32
        )
        scores = scores * score_scale
        positions = offset + jnp.arange(tok_rows, dtype=jnp.int32)
        causal = jnp.arange(length, dtype=jnp.int32)[None, :] <= positions[:, None]
        scores = jnp.where(causal[None], scores, -1e30)
        highest = jnp.max(scores, axis=-1, keepdims=True)
        exponent = jnp.exp(scores - highest)
        probabilities = exponent / jnp.sum(exponent, axis=-1, keepdims=True)
        context = jnp.einsum(
            "hqk,kd->qhd",
            probabilities.astype(jnp.bfloat16),
            value_vectors,
            preferred_element_type=jnp.float32,
        )
        context = context.astype(jnp.bfloat16).reshape(tok_rows, head_count * head_size)
        attended = jnp.concatenate(
            [jnp.dot(context, side, preferred_element_type=jnp.float32) for side in outer], axis=1
        )
        return (attended, key_vectors, value_vectors)

    keys = jnp.zeros((length, head_size), jnp.bfloat16)
    values = jnp.zeros((length, head_size), jnp.bfloat16)
    leading = layer == 0
    first_block = jnp.int32(0)
    first_rows = tokens[0]
    mixed = lax.cond(
        leading,
        lambda rows: mixture(rows, first_block, own),
        lambda rows: jnp.zeros((tok_rows, model_width), jnp.float32),
        first_rows,
    )
    full, here_matrices = lax.optimization_barrier((full, here_matrices))
    inner, outer = attention_weights(full)

    def first_attend(arrays):
        rows, mixed, keys, values = arrays
        attended, keys, values = attend(rows, first_block, keys, values, inner, outer)
        output_rows = (rows.astype(jnp.float32) + attended + mixed).astype(jnp.bfloat16)
        return (output_rows, keys, values)

    output_rows, keys, values = lax.cond(
        leading,
        first_attend,
        lambda arrays: (arrays[0], arrays[2], arrays[3]),
        (first_rows, mixed, keys, values),
    )
    tick_count = micro_count + section_count - 1
    stored = jnp.zeros((tick_count, tok_rows, model_width), jnp.bfloat16)
    stored = lax.dynamic_update_index_in_dim(stored, output_rows, 0, 0)

    def advance(tick_index, state_carry):
        output_rows, keys, values, stored = state_carry
        inbound = lax.ppermute(output_rows, "section", RELAY)
        block_index = tick_index - layer
        active = (block_index >= 0) & (block_index < micro_count)
        block = jnp.clip(block_index, 0, micro_count - 1)

        def work(arrays):
            inbound, keys, values = arrays
            held = lax.dynamic_index_in_dim(tokens, block, 0, keepdims=False)
            layer_input = jnp.where(layer == 0, held, inbound)
            mixed = mixture(layer_input, block, here_matrices)
            attended, keys, values = attend(layer_input, block, keys, values, inner, outer)
            output_rows = layer_input.astype(jnp.float32) + attended + mixed
            return (output_rows.astype(jnp.bfloat16), keys, values)

        output_rows, keys, values = lax.cond(
            active, work, lambda arrays: arrays, (inbound, keys, values)
        )
        stored = lax.dynamic_update_index_in_dim(stored, output_rows, tick_index, 0)
        return (output_rows, keys, values, stored)

    finals = lax.fori_loop(1, tick_count, advance, (output_rows, keys, values, stored))
    results = lax.dynamic_slice_in_dim(finals[3], layer, micro_count, 0)
    returned_home = lax.ppermute(results, "section", HOME)
    return jnp.where(here, results, returned_home)[None]


def solution(mesh):
    placed = (
        P(None, "expert", None),
        P("section", None),
        P("section", None),
        P("section", "expert", None),
        P("section", "expert", None),
        P("section", "expert", None),
        P("section", "expert", None),
        P("section", "expert", None, None),
        P("section", "expert", None, None),
        P("section", "expert", None, None),
        P("section", None, "expert", None),
        P("section", None, "expert", None),
    )
    return jax.shard_map(
        shards,
        mesh=mesh,
        in_specs=placed,
        out_specs=P("section", None, "expert", None),
        check_vma=False,
    )
```

```python
import jax
import jax.numpy as jnp
from jax import lax
from jax.experimental import pallas as pl
from jax.experimental.pallas import tpu as pltpu
from jax.sharding import PartitionSpec as P

epsilon = 1e-06

POSITION = (0, 6, 2, 4, 7, 3, 1, 5)
LAYER_AT = tuple(POSITION.index(place) for place in range(8))
MOVES = [(layer, place) for layer, place in enumerate(POSITION) if layer != place]
HOME = [(place, layer) for layer, place in MOVES]
RELAY = [(POSITION[layer], POSITION[layer + 1]) for layer in range(7)]

SPAN = 352
FLIGHT = 3


def rms_normed(wide, gain_vector):
    scale = lax.rsqrt(jnp.mean(wide * wide, axis=-1, keepdims=True) + epsilon)
    return (wide * scale * gain_vector).astype(jnp.bfloat16)


def expert_kernel(
    rows_ref, gate_hbm, up_hbm, down_hbm, out_ref, gate_buf, up_buf, down_buf, hidden_buf, sems
):
    hidden_width = down_buf.shape[0]
    spans = [
        pl.ds(first, min(SPAN, hidden_width - first)) for first in range(0, hidden_width, SPAN)
    ]
    sources = []
    for span in spans:
        sources.append((gate_hbm, gate_buf, span))
        sources.append((up_hbm, up_buf, span))
    for span in spans:
        sources.append((down_hbm, down_buf, span))
    copies = [
        pltpu.make_async_copy(source.at[span, :], target.at[span, :], sems.at[number])
        for number, (source, target, span) in enumerate(sources)
    ]
    for copy in copies[:FLIGHT]:
        copy.start()

    def arrive(number):
        copies[number].wait()
        if number + FLIGHT < len(copies):
            copies[number + FLIGHT].start()

    across = (((1,), (1,)), ((), ()))
    rows = rows_ref[...]
    for number, span in enumerate(spans):
        arrive(2 * number)
        gated = lax.dot_general(
            rows, gate_buf[span, :], across, preferred_element_type=jnp.float32
        )
        arrive(2 * number + 1)
        lifted = lax.dot_general(rows, up_buf[span, :], across, preferred_element_type=jnp.float32)
        hidden = gated * jax.nn.sigmoid(gated) * lifted
        hidden_buf[:, span] = hidden.astype(jnp.bfloat16)
    for number in range(len(spans)):
        arrive(2 * len(spans) + number)
    out_ref[...] = jnp.dot(
        hidden_buf[...], down_buf[...], preferred_element_type=jnp.float32
    ).astype(jnp.bfloat16)


def expert_rows(rows, matrices):
    count, model_width = rows.shape
    hidden_width = matrices[2].shape[0]
    vmem = pl.BlockSpec(memory_space=pltpu.VMEM)
    anywhere = pl.BlockSpec(memory_space=pl.ANY)
    copy_count = 3 * -(-hidden_width // SPAN)
    return pl.pallas_call(
        expert_kernel,
        out_shape=jax.ShapeDtypeStruct((count, model_width), jnp.bfloat16),
        in_specs=[vmem, anywhere, anywhere, anywhere],
        out_specs=vmem,
        scratch_shapes=[
            pltpu.VMEM((hidden_width, model_width), jnp.bfloat16),
            pltpu.VMEM((hidden_width, model_width), jnp.bfloat16),
            pltpu.VMEM((hidden_width, model_width), jnp.bfloat16),
            pltpu.VMEM((count, hidden_width), jnp.bfloat16),
            pltpu.SemaphoreType.DMA((copy_count,)),
        ],
        compiler_params=pltpu.CompilerParams(vmem_limit_bytes=24 * 2**20),
        cost_estimate=pl.CostEstimate(
            flops=6 * count * model_width * hidden_width,
            bytes_accessed=6 * model_width * hidden_width + 4 * count * model_width,
            transcendentals=count * hidden_width,
        ),
        name="experts",
    )(rows, *matrices)


def route_tables(picks, codes, expert_count, capacity):
    micro_count, tok_rows, pick_count = picks.shape
    flat_ids = picks.reshape(micro_count, tok_rows * pick_count)
    experts = jnp.arange(expert_count, dtype=jnp.int32)
    matches = (flat_ids[:, :, None] == experts[None, None, :]).astype(jnp.float32)
    order = jnp.arange(tok_rows * pick_count, dtype=jnp.int32)
    earlier = (order[:, None] > order[None, :]).astype(jnp.float32)
    before = jnp.einsum("ij,mje->mie", earlier, matches)
    slot_ranks = jnp.sum(before * matches, axis=2).astype(jnp.int32)
    columns = (flat_ids * capacity + slot_ranks).reshape(micro_count, tok_rows, pick_count)
    slots = jnp.arange(expert_count * capacity, dtype=jnp.int32)
    pick_weights = codes.astype(jnp.float32) / 64.0
    scatter_table = jnp.zeros((micro_count, tok_rows, expert_count * capacity), jnp.float32)
    combine_table = scatter_table
    for pick in range(pick_count):
        onehot = (columns[:, :, pick, None] == slots[None, None, :]).astype(jnp.float32)
        scatter_table = scatter_table + onehot
        combine_table = combine_table + onehot * pick_weights[:, :, pick, None]
    return (scatter_table.astype(jnp.bfloat16), combine_table.astype(jnp.bfloat16))


def shards(
    tokens,
    attn_norm,
    moe_norm,
    query_weight,
    key_weight,
    value_weight,
    out_weight,
    gate_proj,
    up_proj,
    down_proj,
    routes,
    weights_code,
):
    section_count = lax.axis_size("section")
    place = lax.axis_index("section")
    expert_devices = lax.axis_size("expert")
    micro_count, tok_rows, model_width = tokens.shape
    pick_count = routes.shape[3]
    expert_count = expert_devices * gate_proj.shape[1]
    capacity = min(tok_rows, tok_rows * pick_count * 4 // (3 * expert_count))
    layer = jnp.asarray(LAYER_AT, jnp.int32)[place]
    here = layer == place

    def relocated(value):
        return jnp.where(here, value, lax.ppermute(value, "section", MOVES))

    head_size = key_weight.shape[-1]
    head_count = query_weight.shape[-1] // head_size
    half = model_width // 2
    out_shard = out_weight[0]
    packed = jnp.concatenate(
        [
            query_weight[0],
            key_weight[0],
            value_weight[0],
            jnp.concatenate([out_shard[:, :half], out_shard[:, half:]], axis=0),
        ],
        axis=1,
    )
    full = lax.all_gather(relocated(packed), "expert", axis=0, tiled=True)
    tables = relocated(jnp.concatenate([routes[0], weights_code[0]], axis=-1))
    gains = relocated(jnp.concatenate([attn_norm, moe_norm], axis=0))
    attn_gain, moe_gain = gains[0], gains[1]
    scatter_tables, combine_tables = route_tables(
        tables[:, :, :pick_count], tables[:, :, pick_count:], expert_count, capacity
    )
    scatter_tables, combine_tables = lax.optimization_barrier((scatter_tables, combine_tables))
    own = (gate_proj[0, 0].T, up_proj[0, 0].T, down_proj[0, 0])
    here_matrices = tuple(relocated(value) for value in own)

    score_width = (head_count + 2) * head_size
    length = micro_count * tok_rows
    score_scale = head_size ** (-0.5)

    def attention_weights(full):
        rows = out_shard.shape[0]
        halves = full.reshape(expert_devices, 2, rows, score_width + half)
        outer = tuple(
            halves[:, side, :, score_width:].reshape(expert_devices * rows, half)
            for side in range(2)
        )
        return (full[:, :score_width], outer)

    def mixture(layer_input, block, matrices):
        wide = layer_input.astype(jnp.float32)
        normed = rms_normed(wide, moe_gain)
        scatter_table = lax.dynamic_index_in_dim(scatter_tables, block, 0, keepdims=False)
        combine_table = lax.dynamic_index_in_dim(combine_tables, block, 0, keepdims=False)
        outgoing = jnp.einsum("te,td->ed", scatter_table, normed, preferred_element_type=jnp.float32)
        outgoing = outgoing.astype(jnp.bfloat16).reshape(expert_count, capacity, model_width)
        arrived = lax.all_to_all(outgoing, "expert", split_axis=0, concat_axis=0, tiled=True)
        produced = expert_rows(arrived.reshape(-1, model_width), matrices)
        produced = produced.reshape(arrived.shape)
        returned = lax.all_to_all(produced, "expert", split_axis=0, concat_axis=0, tiled=True)
        return jnp.dot(
            combine_table, returned.reshape(-1, model_width), preferred_element_type=jnp.float32
        )

    def attend(layer_input, block, old_keys, old_values, inner, outer):
        normed = rms_normed(layer_input.astype(jnp.float32), attn_gain)
        projected = jnp.dot(normed, inner, preferred_element_type=jnp.float32)
        projected = projected.astype(jnp.bfloat16)
        query_rows = projected[:, : head_count * head_size]
        query_rows = query_rows.reshape(tok_rows, head_count, head_size)
        new_keys = projected[:, head_count * head_size : (head_count + 1) * head_size]
        new_values = projected[:, (head_count + 1) * head_size :]
        offset = block * tok_rows
        key_vectors = lax.dynamic_update_slice_in_dim(old_keys, new_keys, offset, 0)
        value_vectors = lax.dynamic_update_slice_in_dim(old_values, new_values, offset, 0)
        scores = jnp.einsum(
            "qhd,kd->hqk", query_rows, key_vectors, preferred_element_type=jnp.float32
        )
        scores = scores * score_scale
        positions = offset + jnp.arange(tok_rows, dtype=jnp.int32)
        causal = jnp.arange(length, dtype=jnp.int32)[None, :] <= positions[:, None]
        scores = jnp.where(causal[None], scores, -1e30)
        highest = jnp.max(scores, axis=-1, keepdims=True)
        exponent = jnp.exp(scores - highest)
        probabilities = exponent / jnp.sum(exponent, axis=-1, keepdims=True)
        context = jnp.einsum(
            "hqk,kd->qhd",
            probabilities.astype(jnp.bfloat16),
            value_vectors,
            preferred_element_type=jnp.float32,
        )
        context = context.astype(jnp.bfloat16).reshape(tok_rows, head_count * head_size)
        attended = jnp.concatenate(
            [jnp.dot(context, side, preferred_element_type=jnp.float32) for side in outer], axis=1
        )
        return (attended, key_vectors, value_vectors)

    keys = jnp.zeros((length, head_size), jnp.bfloat16)
    values = jnp.zeros((length, head_size), jnp.bfloat16)
    leading = layer == 0
    first_block = jnp.int32(0)
    first_rows = tokens[0]
    mixed = lax.cond(
        leading,
        lambda rows: mixture(rows, first_block, own),
        lambda rows: jnp.zeros((tok_rows, model_width), jnp.float32),
        first_rows,
    )
    full, here_matrices = lax.optimization_barrier((full, here_matrices))
    inner, outer = attention_weights(full)

    def first_attend(arrays):
        rows, mixed, keys, values = arrays
        attended, keys, values = attend(rows, first_block, keys, values, inner, outer)
        return (rows.astype(jnp.float32) + attended + mixed, keys, values)

    nothing = jnp.zeros((tok_rows, model_width), jnp.float32)
    total, keys, values = lax.cond(
        leading,
        first_attend,
        lambda arrays: (nothing, arrays[2], arrays[3]),
        (first_rows, mixed, keys, values),
    )
    tick_count = micro_count + section_count - 1
    stored = jnp.zeros((tick_count, tok_rows, model_width), jnp.bfloat16)
    output_rows = total.astype(jnp.bfloat16)

    def advance(tick_index, state_carry):
        output_rows, keys, values, stored = state_carry
        inbound = lax.ppermute(output_rows, "section", RELAY)
        stored = lax.dynamic_update_index_in_dim(stored, output_rows, tick_index - 1, 0)
        block_index = tick_index - layer
        active = (block_index >= 0) & (block_index < micro_count)
        block = jnp.clip(block_index, 0, micro_count - 1)

        def work(arrays):
            inbound, keys, values = arrays
            held = lax.dynamic_index_in_dim(tokens, block, 0, keepdims=False)
            layer_input = jnp.where(layer == 0, held, inbound)
            mixed = mixture(layer_input, block, here_matrices)
            attended, keys, values = attend(layer_input, block, keys, values, inner, outer)
            output_rows = layer_input.astype(jnp.float32) + attended + mixed
            return (output_rows, keys, values)

        total, keys, values = lax.cond(
            active, work, lambda arrays: (nothing, *arrays[1:]), (inbound, keys, values)
        )
        return (total.astype(jnp.bfloat16), keys, values, stored)

    finals = lax.fori_loop(1, tick_count, advance, (output_rows, keys, values, stored))
    stored = lax.dynamic_update_index_in_dim(finals[3], finals[0], tick_count - 1, 0)
    results = lax.dynamic_slice_in_dim(stored, layer, micro_count, 0)
    returned_home = lax.ppermute(results, "section", HOME)
    return jnp.where(here, results, returned_home)[None]


def solution(mesh):
    placed = (
        P(None, "expert", None),
        P("section", None),
        P("section", None),
        P("section", "expert", None),
        P("section", "expert", None),
        P("section", "expert", None),
        P("section", "expert", None),
        P("section", "expert", None, None),
        P("section", "expert", None, None),
        P("section", "expert", None, None),
        P("section", None, "expert", None),
        P("section", None, "expert", None),
    )
    return jax.shard_map(
        shards,
        mesh=mesh,
        in_specs=placed,
        out_specs=P("section", None, "expert", None),
        check_vma=False,
    )
```

```python
import jax
import jax.numpy as jnp
from jax import lax
from jax.experimental import pallas as pl
from jax.experimental.pallas import tpu as pltpu
from jax.sharding import PartitionSpec as P

epsilon = 1e-06

POSITION = (0, 6, 2, 4, 7, 3, 1, 5)
LAYER_AT = tuple(POSITION.index(place) for place in range(8))
MOVES = [(layer, place) for layer, place in enumerate(POSITION) if layer != place]
HOME = [(place, layer) for layer, place in MOVES]
RELAY = [(POSITION[layer], POSITION[layer + 1]) for layer in range(7)]

SPAN = 1024
FLIGHT = 2


def rms_normed(wide, gain_vector):
    scale = lax.rsqrt(jnp.mean(wide * wide, axis=-1, keepdims=True) + epsilon)
    return (wide * scale * gain_vector).astype(jnp.bfloat16)


def expert_kernel(
    rows_ref,
    gate_hbm,
    up_hbm,
    down_hbm,
    attn_ref,
    out_ref,
    passed_ref,
    gate_buf,
    up_buf,
    down_buf,
    hidden_buf,
    sems,
):
    passed_ref[...] = attn_ref[...]
    hidden_width = down_buf.shape[0]
    spans = [
        pl.ds(first, min(SPAN, hidden_width - first)) for first in range(0, hidden_width, SPAN)
    ]
    sources = []
    for span in spans:
        sources.append((gate_hbm, gate_buf, span))
        sources.append((up_hbm, up_buf, span))
    for span in spans:
        sources.append((down_hbm, down_buf, span))
    copies = [
        pltpu.make_async_copy(source.at[span, :], target.at[span, :], sems.at[number])
        for number, (source, target, span) in enumerate(sources)
    ]
    for copy in copies[:FLIGHT]:
        copy.start()

    def arrive(number):
        copies[number].wait()
        if number + FLIGHT < len(copies):
            copies[number + FLIGHT].start()

    across = (((1,), (1,)), ((), ()))
    rows = rows_ref[...]
    for number, span in enumerate(spans):
        arrive(2 * number)
        gated = lax.dot_general(
            rows, gate_buf[span, :], across, preferred_element_type=jnp.float32
        )
        arrive(2 * number + 1)
        lifted = lax.dot_general(rows, up_buf[span, :], across, preferred_element_type=jnp.float32)
        hidden = gated * jax.nn.sigmoid(gated) * lifted
        hidden_buf[:, span] = hidden.astype(jnp.bfloat16)
    for number in range(len(spans)):
        arrive(2 * len(spans) + number)
    out_ref[...] = jnp.dot(
        hidden_buf[...], down_buf[...], preferred_element_type=jnp.float32
    ).astype(jnp.bfloat16)


def expert_rows(rows, matrices, attn_rows):
    count, model_width = rows.shape
    hidden_width = matrices[2].shape[0]
    vmem = pl.BlockSpec(memory_space=pltpu.VMEM)
    anywhere = pl.BlockSpec(memory_space=pl.ANY)
    copy_count = 3 * -(-hidden_width // SPAN)
    return pl.pallas_call(
        expert_kernel,
        out_shape=[
            jax.ShapeDtypeStruct((count, model_width), jnp.bfloat16),
            jax.ShapeDtypeStruct(attn_rows.shape, attn_rows.dtype),
        ],
        in_specs=[vmem, anywhere, anywhere, anywhere, vmem],
        out_specs=[vmem, vmem],
        scratch_shapes=[
            pltpu.VMEM((hidden_width, model_width), jnp.bfloat16),
            pltpu.VMEM((hidden_width, model_width), jnp.bfloat16),
            pltpu.VMEM((hidden_width, model_width), jnp.bfloat16),
            pltpu.VMEM((count, hidden_width), jnp.bfloat16),
            pltpu.SemaphoreType.DMA((copy_count,)),
        ],
        compiler_params=pltpu.CompilerParams(vmem_limit_bytes=24 * 2**20),
        cost_estimate=pl.CostEstimate(
            flops=6 * count * model_width * hidden_width,
            bytes_accessed=6 * model_width * hidden_width + 4 * count * model_width,
            transcendentals=count * hidden_width,
        ),
        name="experts",
    )(rows, *matrices, attn_rows)


def send_kernel(
    state_ref, inbound_ref, tokens_hbm, gain_ref, table_ref, out_ref, rows_ref, attn_ref, sem
):
    leading, block = state_ref[0], state_ref[1]

    @pl.when(leading != 0)
    def _():
        copy = pltpu.make_async_copy(tokens_hbm.at[block], rows_ref, sem)
        copy.start()
        copy.wait()

    @pl.when(leading == 0)
    def _():
        rows_ref[...] = inbound_ref[...]

    wide = rows_ref[...].astype(jnp.float32)
    scaled = wide * lax.rsqrt(jnp.mean(wide * wide, axis=-1, keepdims=True) + epsilon)
    attn_ref[...] = (scaled * gain_ref[0:1, :]).astype(jnp.bfloat16)
    normed = (scaled * gain_ref[1:2, :]).astype(jnp.bfloat16)
    out_ref[...] = jnp.dot(
        table_ref[block], normed, preferred_element_type=jnp.float32
    ).astype(jnp.bfloat16)


def rows_to_send(state, inbound, tokens, gain, tables):
    vmem = pl.BlockSpec(memory_space=pltpu.VMEM)
    slot_count = tables.shape[1]
    tok_rows, model_width = inbound.shape
    return pl.pallas_call(
        send_kernel,
        out_shape=[
            jax.ShapeDtypeStruct((slot_count, model_width), jnp.bfloat16),
            jax.ShapeDtypeStruct((tok_rows, model_width), jnp.bfloat16),
            jax.ShapeDtypeStruct((tok_rows, model_width), jnp.bfloat16),
        ],
        in_specs=[
            pl.BlockSpec(memory_space=pltpu.SMEM),
            vmem,
            pl.BlockSpec(memory_space=pl.ANY),
            vmem,
            vmem,
        ],
        out_specs=[vmem] * 3,
        scratch_shapes=[pltpu.SemaphoreType.DMA],
        compiler_params=pltpu.CompilerParams(vmem_limit_bytes=12 * 2**20),
        cost_estimate=pl.CostEstimate(
            flops=2 * slot_count * tok_rows * model_width,
            bytes_accessed=2 * (slot_count + 3 * tok_rows) * model_width,
            transcendentals=tok_rows,
        ),
        name="send",
    )(state, inbound, tokens, gain, tables)


def route_tables(picks, codes, expert_count, capacity):
    micro_count, tok_rows, pick_count = picks.shape
    flat_ids = picks.reshape(micro_count, tok_rows * pick_count)
    experts = jnp.arange(expert_count, dtype=jnp.int32)
    matches = (flat_ids[:, :, None] == experts[None, None, :]).astype(jnp.float32)
    order = jnp.arange(tok_rows * pick_count, dtype=jnp.int32)
    earlier = (order[:, None] > order[None, :]).astype(jnp.float32)
    before = jnp.einsum("ij,mje->mie", earlier, matches)
    slot_ranks = jnp.sum(before * matches, axis=2).astype(jnp.int32)
    columns = (flat_ids * capacity + slot_ranks).reshape(micro_count, tok_rows, pick_count)
    slots = jnp.arange(expert_count * capacity, dtype=jnp.int32)
    pick_weights = codes.astype(jnp.float32) / 64.0
    scatter_table = jnp.zeros((micro_count, tok_rows, expert_count * capacity), jnp.float32)
    combine_table = scatter_table
    for pick in range(pick_count):
        onehot = (columns[:, :, pick, None] == slots[None, None, :]).astype(jnp.float32)
        scatter_table = scatter_table + onehot
        combine_table = combine_table + onehot * pick_weights[:, :, pick, None]
    return (scatter_table.astype(jnp.bfloat16), combine_table.astype(jnp.bfloat16))


def shards(
    tokens,
    attn_norm,
    moe_norm,
    query_weight,
    key_weight,
    value_weight,
    out_weight,
    gate_proj,
    up_proj,
    down_proj,
    routes,
    weights_code,
):
    section_count = lax.axis_size("section")
    place = lax.axis_index("section")
    expert_devices = lax.axis_size("expert")
    micro_count, tok_rows, model_width = tokens.shape
    pick_count = routes.shape[3]
    expert_count = expert_devices * gate_proj.shape[1]
    capacity = min(tok_rows, tok_rows * pick_count * 4 // (3 * expert_count))
    layer = jnp.asarray(LAYER_AT, jnp.int32)[place]
    here = layer == place

    def relocated(value):
        return jnp.where(here, value, lax.ppermute(value, "section", MOVES))

    head_size = key_weight.shape[-1]
    head_count = query_weight.shape[-1] // head_size
    half = model_width // 2
    out_shard = out_weight[0]
    packed = jnp.concatenate(
        [
            query_weight[0],
            key_weight[0],
            value_weight[0],
            jnp.concatenate([out_shard[:, :half], out_shard[:, half:]], axis=0),
        ],
        axis=1,
    )
    full = lax.all_gather(relocated(packed), "expert", axis=0, tiled=True)
    tables = relocated(jnp.concatenate([routes[0], weights_code[0]], axis=-1))
    gains = relocated(jnp.concatenate([attn_norm, moe_norm], axis=0))
    attn_gain = gains[0]
    scatter_tables, combine_tables = route_tables(
        tables[:, :, :pick_count], tables[:, :, pick_count:], expert_count, capacity
    )
    scatter_tables, combine_tables = lax.optimization_barrier(
        (jnp.swapaxes(scatter_tables, 1, 2), combine_tables)
    )
    own = (gate_proj[0, 0].T, up_proj[0, 0].T, down_proj[0, 0])
    here_matrices = tuple(relocated(value) for value in own)

    score_width = (head_count + 2) * head_size
    length = micro_count * tok_rows
    score_scale = head_size ** (-0.5)

    def attention_weights(full):
        rows = out_shard.shape[0]
        halves = full.reshape(expert_devices, 2, rows, score_width + half)
        outer = tuple(
            halves[:, side, :, score_width:].reshape(expert_devices * rows, half)
            for side in range(2)
        )
        return (full[:, :score_width], outer)

    def mixture(inbound, leads, block, matrices):
        combine_table = lax.dynamic_index_in_dim(combine_tables, block, 0, keepdims=False)
        state = jnp.stack([leads.astype(jnp.int32), block])
        outgoing, layer_input, attn_rows = rows_to_send(
            state, inbound, tokens, gains, scatter_tables
        )
        outgoing = outgoing.reshape(expert_count, capacity, model_width)
        arrived = lax.all_to_all(outgoing, "expert", split_axis=0, concat_axis=0, tiled=True)
        produced, attn_rows = expert_rows(arrived.reshape(-1, model_width), matrices, attn_rows)
        produced = produced.reshape(arrived.shape)
        returned = lax.all_to_all(produced, "expert", split_axis=0, concat_axis=0, tiled=True)
        mixed = jnp.dot(
            combine_table, returned.reshape(-1, model_width), preferred_element_type=jnp.float32
        )
        return (mixed, layer_input, attn_rows)

    def attend(normed, block, old_keys, old_values, inner, outer):
        projected = jnp.dot(normed, inner, preferred_element_type=jnp.float32)
        projected = projected.astype(jnp.bfloat16)
        query_rows = projected[:, : head_count * head_size]
        query_rows = query_rows.reshape(tok_rows, head_count, head_size)
        new_keys = projected[:, head_count * head_size : (head_count + 1) * head_size]
        new_values = projected[:, (head_count + 1) * head_size :]
        offset = block * tok_rows
        key_vectors = lax.dynamic_update_slice_in_dim(old_keys, new_keys, offset, 0)
        value_vectors = lax.dynamic_update_slice_in_dim(old_values, new_values, offset, 0)
        scores = jnp.einsum(
            "qhd,kd->hqk", query_rows, key_vectors, preferred_element_type=jnp.float32
        )
        scores = scores * score_scale
        positions = offset + jnp.arange(tok_rows, dtype=jnp.int32)
        causal = jnp.arange(length, dtype=jnp.int32)[None, :] <= positions[:, None]
        scores = jnp.where(causal[None], scores, -1e30)
        highest = jnp.max(scores, axis=-1, keepdims=True)
        exponent = jnp.exp(scores - highest)
        probabilities = exponent / jnp.sum(exponent, axis=-1, keepdims=True)
        context = jnp.einsum(
            "hqk,kd->qhd",
            probabilities.astype(jnp.bfloat16),
            value_vectors,
            preferred_element_type=jnp.float32,
        )
        context = context.astype(jnp.bfloat16).reshape(tok_rows, head_count * head_size)
        attended = jnp.concatenate(
            [jnp.dot(context, side, preferred_element_type=jnp.float32) for side in outer], axis=1
        )
        return (attended, key_vectors, value_vectors)

    keys = jnp.zeros((length, head_size), jnp.bfloat16)
    values = jnp.zeros((length, head_size), jnp.bfloat16)
    leading = layer == 0
    first_block = jnp.int32(0)
    first_rows = tokens[0]
    mixed = lax.cond(
        leading,
        lambda rows: mixture(rows, jnp.bool_(False), first_block, own)[0],
        lambda rows: jnp.zeros((tok_rows, model_width), jnp.float32),
        first_rows,
    )
    full, here_matrices = lax.optimization_barrier((full, here_matrices))
    inner, outer = attention_weights(full)

    def first_attend(arrays):
        rows, mixed, keys, values = arrays
        normed = rms_normed(rows.astype(jnp.float32), attn_gain)
        attended, keys, values = attend(normed, first_block, keys, values, inner, outer)
        return (rows.astype(jnp.float32) + attended + mixed, keys, values)

    nothing = jnp.zeros((tok_rows, model_width), jnp.float32)
    total, keys, values = lax.cond(
        leading,
        first_attend,
        lambda arrays: (nothing, arrays[2], arrays[3]),
        (first_rows, mixed, keys, values),
    )
    tick_count = micro_count + section_count - 1
    stored = jnp.zeros((tick_count, tok_rows, model_width), jnp.bfloat16)
    output_rows = total.astype(jnp.bfloat16)

    def advance(tick_index, state_carry):
        output_rows, keys, values, stored = state_carry
        inbound = lax.ppermute(output_rows, "section", RELAY)
        stored = lax.dynamic_update_index_in_dim(stored, output_rows, tick_index - 1, 0)
        block_index = tick_index - layer
        active = (block_index >= 0) & (block_index < micro_count)
        block = jnp.clip(block_index, 0, micro_count - 1)

        def work(arrays):
            inbound, keys, values = arrays
            mixed, layer_input, attn_rows = mixture(inbound, layer == 0, block, here_matrices)
            attended, keys, values = attend(attn_rows, block, keys, values, inner, outer)
            output_rows = layer_input.astype(jnp.float32) + attended + mixed
            return (output_rows, keys, values)

        total, keys, values = lax.cond(
            active, work, lambda arrays: (nothing, *arrays[1:]), (inbound, keys, values)
        )
        return (total.astype(jnp.bfloat16), keys, values, stored)

    finals = lax.fori_loop(1, tick_count, advance, (output_rows, keys, values, stored))
    stored = lax.dynamic_update_index_in_dim(finals[3], finals[0], tick_count - 1, 0)
    results = lax.dynamic_slice_in_dim(stored, layer, micro_count, 0)
    returned_home = lax.ppermute(results, "section", HOME)
    return jnp.where(here, results, returned_home)[None]


def solution(mesh):
    placed = (
        P(None, "expert", None),
        P("section", None),
        P("section", None),
        P("section", "expert", None),
        P("section", "expert", None),
        P("section", "expert", None),
        P("section", "expert", None),
        P("section", "expert", None, None),
        P("section", "expert", None, None),
        P("section", "expert", None, None),
        P("section", None, "expert", None),
        P("section", None, "expert", None),
    )
    return jax.shard_map(
        shards,
        mesh=mesh,
        in_specs=placed,
        out_specs=P("section", None, "expert", None),
        check_vma=False,
    )
```

```python
import jax
import jax.numpy as jnp
from jax import lax
from jax.experimental import pallas as pl
from jax.experimental.pallas import tpu as pltpu
from jax.sharding import PartitionSpec as P

epsilon = 1e-06

POSITION = (0, 6, 2, 4, 7, 3, 1, 5)
LAYER_AT = tuple(POSITION.index(place) for place in range(8))
MOVES = [(layer, place) for layer, place in enumerate(POSITION) if layer != place]
HOME = [(place, layer) for layer, place in MOVES]
RELAY = [(POSITION[layer], POSITION[layer + 1]) for layer in range(7)]

SPAN = 1024
FLIGHT = 2


def rms_normed(wide, gain_vector):
    scale = lax.rsqrt(jnp.mean(wide * wide, axis=-1, keepdims=True) + epsilon)
    return (wide * scale * gain_vector).astype(jnp.bfloat16)


def expert_kernel(
    rows_ref,
    gate_hbm,
    up_hbm,
    down_hbm,
    attn_ref,
    out_ref,
    passed_ref,
    gate_buf,
    up_buf,
    down_buf,
    hidden_buf,
    sems,
):
    passed_ref[...] = attn_ref[...]
    hidden_width = down_buf.shape[0]
    spans = [
        pl.ds(first, min(SPAN, hidden_width - first)) for first in range(0, hidden_width, SPAN)
    ]
    sources = []
    for span in spans:
        sources.append((gate_hbm, gate_buf, span))
        sources.append((up_hbm, up_buf, span))
    for span in spans:
        sources.append((down_hbm, down_buf, span))
    copies = [
        pltpu.make_async_copy(source.at[span, :], target.at[span, :], sems.at[number])
        for number, (source, target, span) in enumerate(sources)
    ]
    for copy in copies[:FLIGHT]:
        copy.start()

    def arrive(number):
        copies[number].wait()
        if number + FLIGHT < len(copies):
            copies[number + FLIGHT].start()

    across = (((1,), (1,)), ((), ()))
    rows = rows_ref[...]
    for number, span in enumerate(spans):
        arrive(2 * number)
        gated = lax.dot_general(
            rows, gate_buf[span, :], across, preferred_element_type=jnp.float32
        )
        arrive(2 * number + 1)
        lifted = lax.dot_general(rows, up_buf[span, :], across, preferred_element_type=jnp.float32)
        hidden = gated * jax.nn.sigmoid(gated) * lifted
        hidden_buf[:, span] = hidden.astype(jnp.bfloat16)
    for number in range(len(spans)):
        arrive(2 * len(spans) + number)
    out_ref[...] = jnp.dot(
        hidden_buf[...], down_buf[...], preferred_element_type=jnp.float32
    ).astype(jnp.bfloat16)


def expert_rows(rows, matrices, attn_rows):
    count, model_width = rows.shape
    hidden_width = matrices[2].shape[0]
    vmem = pl.BlockSpec(memory_space=pltpu.VMEM)
    anywhere = pl.BlockSpec(memory_space=pl.ANY)
    copy_count = 3 * -(-hidden_width // SPAN)
    return pl.pallas_call(
        expert_kernel,
        out_shape=[
            jax.ShapeDtypeStruct((count, model_width), jnp.bfloat16),
            jax.ShapeDtypeStruct(attn_rows.shape, attn_rows.dtype),
        ],
        in_specs=[vmem, anywhere, anywhere, anywhere, vmem],
        out_specs=[vmem, vmem],
        scratch_shapes=[
            pltpu.VMEM((hidden_width, model_width), jnp.bfloat16),
            pltpu.VMEM((hidden_width, model_width), jnp.bfloat16),
            pltpu.VMEM((hidden_width, model_width), jnp.bfloat16),
            pltpu.VMEM((count, hidden_width), jnp.bfloat16),
            pltpu.SemaphoreType.DMA((copy_count,)),
        ],
        compiler_params=pltpu.CompilerParams(vmem_limit_bytes=24 * 2**20),
        cost_estimate=pl.CostEstimate(
            flops=6 * count * model_width * hidden_width,
            bytes_accessed=6 * model_width * hidden_width + 4 * count * model_width,
            transcendentals=count * hidden_width,
        ),
        name="experts",
    )(rows, *matrices, attn_rows)


def send_kernel(
    layer_ref,
    block_ref,
    inbound_ref,
    tokens_hbm,
    gain_ref,
    table_ref,
    out_ref,
    rows_ref,
    attn_ref,
    sem,
):
    layer, block = layer_ref[0], block_ref[0]

    @pl.when(layer == 0)
    def _():
        copy = pltpu.make_async_copy(tokens_hbm.at[block], rows_ref, sem)
        copy.start()
        copy.wait()

    @pl.when(layer != 0)
    def _():
        rows_ref[...] = inbound_ref[...]

    wide = rows_ref[...].astype(jnp.float32)
    scaled = wide * lax.rsqrt(jnp.mean(wide * wide, axis=-1, keepdims=True) + epsilon)
    attn_ref[...] = (scaled * gain_ref[0:1, :]).astype(jnp.bfloat16)
    normed = (scaled * gain_ref[1:2, :]).astype(jnp.bfloat16)
    out_ref[...] = jnp.dot(
        table_ref[block], normed, preferred_element_type=jnp.float32
    ).astype(jnp.bfloat16)


def rows_to_send(layer, block, inbound, tokens, gain, tables):
    vmem = pl.BlockSpec(memory_space=pltpu.VMEM)
    slot_count = tables.shape[1]
    tok_rows, model_width = inbound.shape
    return pl.pallas_call(
        send_kernel,
        out_shape=[
            jax.ShapeDtypeStruct((slot_count, model_width), jnp.bfloat16),
            jax.ShapeDtypeStruct((tok_rows, model_width), jnp.bfloat16),
            jax.ShapeDtypeStruct((tok_rows, model_width), jnp.bfloat16),
        ],
        in_specs=[
            pl.BlockSpec(memory_space=pltpu.SMEM),
            pl.BlockSpec(memory_space=pltpu.SMEM),
            vmem,
            pl.BlockSpec(memory_space=pl.ANY),
            vmem,
            vmem,
        ],
        out_specs=[vmem] * 3,
        scratch_shapes=[pltpu.SemaphoreType.DMA],
        compiler_params=pltpu.CompilerParams(vmem_limit_bytes=12 * 2**20),
        cost_estimate=pl.CostEstimate(
            flops=2 * slot_count * tok_rows * model_width,
            bytes_accessed=2 * (slot_count + 3 * tok_rows) * model_width,
            transcendentals=tok_rows,
        ),
        name="send",
    )(layer.reshape(1), block.reshape(1), inbound, tokens, gain, tables)


def route_tables(picks, codes, expert_count, capacity):
    micro_count, tok_rows, pick_count = picks.shape
    flat_ids = picks.reshape(micro_count, tok_rows * pick_count)
    experts = jnp.arange(expert_count, dtype=jnp.int32)
    matches = (flat_ids[:, :, None] == experts[None, None, :]).astype(jnp.float32)
    order = jnp.arange(tok_rows * pick_count, dtype=jnp.int32)
    earlier = (order[:, None] > order[None, :]).astype(jnp.float32)
    before = jnp.einsum("ij,mje->mie", earlier, matches)
    slot_ranks = jnp.sum(before * matches, axis=2).astype(jnp.int32)
    columns = (flat_ids * capacity + slot_ranks).reshape(micro_count, tok_rows, pick_count)
    slots = jnp.arange(expert_count * capacity, dtype=jnp.int32)
    pick_weights = codes.astype(jnp.float32) / 64.0
    scatter_table = jnp.zeros((micro_count, tok_rows, expert_count * capacity), jnp.float32)
    combine_table = scatter_table
    for pick in range(pick_count):
        onehot = (columns[:, :, pick, None] == slots[None, None, :]).astype(jnp.float32)
        scatter_table = scatter_table + onehot
        combine_table = combine_table + onehot * pick_weights[:, :, pick, None]
    return (scatter_table.astype(jnp.bfloat16), combine_table.astype(jnp.bfloat16))


def shards(
    tokens,
    attn_norm,
    moe_norm,
    query_weight,
    key_weight,
    value_weight,
    out_weight,
    gate_proj,
    up_proj,
    down_proj,
    routes,
    weights_code,
):
    section_count = lax.axis_size("section")
    place = lax.axis_index("section")
    expert_devices = lax.axis_size("expert")
    micro_count, tok_rows, model_width = tokens.shape
    pick_count = routes.shape[3]
    expert_count = expert_devices * gate_proj.shape[1]
    capacity = min(tok_rows, tok_rows * pick_count * 4 // (3 * expert_count))
    layer = jnp.asarray(LAYER_AT, jnp.int32)[place]
    here = layer == place

    def relocated(value):
        return jnp.where(here, value, lax.ppermute(value, "section", MOVES))

    head_size = key_weight.shape[-1]
    head_count = query_weight.shape[-1] // head_size
    half = model_width // 2
    out_shard = out_weight[0]
    packed = jnp.concatenate(
        [
            query_weight[0],
            key_weight[0],
            value_weight[0],
            jnp.concatenate([out_shard[:, :half], out_shard[:, half:]], axis=0),
        ],
        axis=1,
    )
    full = lax.all_gather(relocated(packed), "expert", axis=0, tiled=True)
    tables = relocated(jnp.concatenate([routes[0], weights_code[0]], axis=-1))
    gains = relocated(jnp.concatenate([attn_norm, moe_norm], axis=0))
    attn_gain = gains[0]
    scatter_tables, combine_tables = route_tables(
        tables[:, :, :pick_count], tables[:, :, pick_count:], expert_count, capacity
    )
    scatter_tables, combine_tables = lax.optimization_barrier(
        (jnp.swapaxes(scatter_tables, 1, 2), combine_tables)
    )
    own = (gate_proj[0, 0].T, up_proj[0, 0].T, down_proj[0, 0])
    here_matrices = tuple(relocated(value) for value in own)

    score_width = (head_count + 2) * head_size
    length = micro_count * tok_rows
    score_scale = head_size ** (-0.5)

    def attention_weights(full):
        rows = out_shard.shape[0]
        halves = full.reshape(expert_devices, 2, rows, score_width + half)
        outer = tuple(
            halves[:, side, :, score_width:].reshape(expert_devices * rows, half)
            for side in range(2)
        )
        return (full[:, :score_width], outer)

    def mixture(inbound, block, matrices):
        combine_table = lax.dynamic_index_in_dim(combine_tables, block, 0, keepdims=False)
        outgoing, layer_input, attn_rows = rows_to_send(
            layer, block, inbound, tokens, gains, scatter_tables
        )
        outgoing = outgoing.reshape(expert_count, capacity, model_width)
        arrived = lax.all_to_all(outgoing, "expert", split_axis=0, concat_axis=0, tiled=True)
        produced, attn_rows = expert_rows(arrived.reshape(-1, model_width), matrices, attn_rows)
        produced = produced.reshape(arrived.shape)
        returned = lax.all_to_all(produced, "expert", split_axis=0, concat_axis=0, tiled=True)
        mixed = jnp.dot(
            combine_table, returned.reshape(-1, model_width), preferred_element_type=jnp.float32
        )
        return (mixed, layer_input, attn_rows)

    def attend(normed, block, old_keys, old_values, inner, outer):
        projected = jnp.dot(normed, inner, preferred_element_type=jnp.float32)
        projected = projected.astype(jnp.bfloat16)
        query_rows = projected[:, : head_count * head_size]
        query_rows = query_rows.reshape(tok_rows, head_count, head_size)
        new_keys = projected[:, head_count * head_size : (head_count + 1) * head_size]
        new_values = projected[:, (head_count + 1) * head_size :]
        offset = block * tok_rows
        key_vectors = lax.dynamic_update_slice_in_dim(old_keys, new_keys, offset, 0)
        value_vectors = lax.dynamic_update_slice_in_dim(old_values, new_values, offset, 0)
        scores = jnp.einsum(
            "qhd,kd->hqk", query_rows, key_vectors, preferred_element_type=jnp.float32
        )
        scores = scores * score_scale
        positions = offset + jnp.arange(tok_rows, dtype=jnp.int32)
        causal = jnp.arange(length, dtype=jnp.int32)[None, :] <= positions[:, None]
        scores = jnp.where(causal[None], scores, -1e30)
        highest = jnp.max(scores, axis=-1, keepdims=True)
        exponent = jnp.exp(scores - highest)
        probabilities = exponent / jnp.sum(exponent, axis=-1, keepdims=True)
        context = jnp.einsum(
            "hqk,kd->qhd",
            probabilities.astype(jnp.bfloat16),
            value_vectors,
            preferred_element_type=jnp.float32,
        )
        context = context.astype(jnp.bfloat16).reshape(tok_rows, head_count * head_size)
        attended = jnp.concatenate(
            [jnp.dot(context, side, preferred_element_type=jnp.float32) for side in outer], axis=1
        )
        return (attended, key_vectors, value_vectors)

    keys = jnp.zeros((length, head_size), jnp.bfloat16)
    values = jnp.zeros((length, head_size), jnp.bfloat16)
    leading = layer == 0
    first_block = jnp.int32(0)
    first_rows = tokens[0]
    mixed = lax.cond(
        leading,
        lambda rows: mixture(rows, first_block, own)[0],
        lambda rows: jnp.zeros((tok_rows, model_width), jnp.float32),
        first_rows,
    )
    full, here_matrices = lax.optimization_barrier((full, here_matrices))
    inner, outer = attention_weights(full)

    def first_attend(arrays):
        rows, mixed, keys, values = arrays
        normed = rms_normed(rows.astype(jnp.float32), attn_gain)
        attended, keys, values = attend(normed, first_block, keys, values, inner, outer)
        return (rows.astype(jnp.float32) + attended + mixed, keys, values)

    nothing = jnp.zeros((tok_rows, model_width), jnp.float32)
    total, keys, values = lax.cond(
        leading,
        first_attend,
        lambda arrays: (nothing, arrays[2], arrays[3]),
        (first_rows, mixed, keys, values),
    )
    tick_count = micro_count + section_count - 1
    stored = jnp.zeros((tick_count, tok_rows, model_width), jnp.bfloat16)
    output_rows = total.astype(jnp.bfloat16)

    def advance(tick_index, inbound, keys, values):
        block_index = tick_index - layer
        active = (block_index >= 0) & (block_index < micro_count)
        block = jnp.clip(block_index, 0, micro_count - 1)

        def work(arrays):
            inbound, keys, values = arrays
            mixed, layer_input, attn_rows = mixture(inbound, block, here_matrices)
            attended, keys, values = attend(attn_rows, block, keys, values, inner, outer)
            output_rows = layer_input.astype(jnp.float32) + attended + mixed
            return (output_rows, keys, values)

        total, keys, values = lax.cond(
            active, work, lambda arrays: (nothing, *arrays[1:]), (inbound, keys, values)
        )
        return (total.astype(jnp.bfloat16), keys, values)

    def tick(tick_index, state_carry):
        output_rows, keys, values, stored = state_carry
        inbound = lax.ppermute(output_rows, "section", RELAY)
        stored = lax.dynamic_update_index_in_dim(stored, output_rows, tick_index - 1, 0)
        return (*advance(tick_index, inbound, keys, values), stored)

    finals = lax.fori_loop(1, tick_count, tick, (output_rows, keys, values, stored))
    stored = lax.dynamic_update_index_in_dim(finals[3], finals[0], tick_count - 1, 0)
    results = lax.dynamic_slice_in_dim(stored, layer, micro_count, 0)
    returned_home = lax.ppermute(results, "section", HOME)
    return jnp.where(here, results, returned_home)[None]


def solution(mesh):
    placed = (
        P(None, "expert", None),
        P("section", None),
        P("section", None),
        P("section", "expert", None),
        P("section", "expert", None),
        P("section", "expert", None),
        P("section", "expert", None),
        P("section", "expert", None, None),
        P("section", "expert", None, None),
        P("section", "expert", None, None),
        P("section", None, "expert", None),
        P("section", None, "expert", None),
    )
    return jax.shard_map(
        shards,
        mesh=mesh,
        in_specs=placed,
        out_specs=P("section", None, "expert", None),
        check_vma=False,
    )
```
